32 devices in a mesh: expert: 4 (over x, core), shard: 8 (over z, y).
Axes of the slice: x: 2, y: 2, z: 4, core: 2. Of those that a mesh axis runs over, the one named last changes fastest.
Arguments:
- train_down: float32 [16, 6400, 4096], P('expert', None, 'shard'), may hold values from -0.109375 to 0.109375
- other_down: bfloat16 [16, 6400, 4096], P('expert', None, 'shard'), may hold values from -0.0390625 to 0.0390625
- router_weight: float32 [4096, 16], P('shard', 'expert'), may hold values from -0.09375 to 0.09375
- router_gain: float32 [4096], P('shard'), may hold values from 0.25 to 1.75
Outputs:
- ready_down: bfloat16 [16, 6400, 4096], P('expert', 'shard')
- scale_down: float32 [16, 6400], P('expert', 'shard')
- serve_router: bfloat16 [4096, 16], replicated
The draws below stay inside these ranges and needn't reach their ends.
All inputs are finite; a program needn't handle non-finite values. Where the reference program divides by a largest or mean magnitude, that divisor is 1e-20 or more.
Results may differ from the reference program's by a relative error of at most 0.001.
Values may be sent and summed in bfloat16 or wider, within the bound.
A program may use at most 256 MiB of HBM per device.

```python
import jax
import jax.numpy as jnp

EXPERTS = 16
D_MODEL = 4096
D_EXPERT = 6400


def spiked(array, rng, source, target, blocks, factor):
    owner, partner = [(jnp.arange(array.shape[axis_at]) // (array.shape[axis_at] // blocks)).reshape([-1 if axis == axis_at else 1 for axis in range(array.ndim)]) for axis_at in (source, target)]
    chosen = jax.random.permutation(rng, blocks)[partner]
    strong = (owner == chosen) | (owner == (partner + blocks // 2) % blocks)
    return jnp.where(strong, factor * array, array)


def block_levels(stream_key, dims, pieces, smallest, high):
    factor_of = 1.0
    for axis_at, parts in pieces:
        draws = jax.random.uniform(jax.random.fold_in(jax.random.fold_in(stream_key, 6), axis_at), (parts,), jnp.float32, smallest / len(pieces), high / len(pieces))
        factor_of = factor_of * jnp.repeat(jnp.exp(draws), dims[axis_at] // parts).reshape((-1,) + (1,) * (len(dims) - 1 - axis_at))
    return factor_of


def noise(key, dims, width, reach, pieces=(), dtype=jnp.bfloat16):
    drawn = width * jax.random.normal(key, dims, jnp.float32)
    if pieces:
        drawn = drawn * block_levels(key, dims, pieces, -0.22, 0.18)
    return jnp.clip(drawn, -reach, reach).astype(dtype)


def noise_with(rng, dims, width, reach, pieces, heavy, dtype=jnp.bfloat16):
    values = width * jax.random.normal(rng, dims, jnp.float32)
    if pieces:
        values = values * block_levels(rng, dims, pieces, -0.22, 0.18)
    return jnp.clip(spiked(values, jax.random.fold_in(rng, 3), *heavy), -reach, reach).astype(dtype)


def setup_inputs(seed: int = 0) -> dict:
    arg_keys = jax.random.split(jax.random.key(seed), 5)
    return {
        "train_down": noise_with(arg_keys[0], (EXPERTS, D_EXPERT, D_MODEL), D_EXPERT ** -0.5, 0.109375, ((0, 4), (2, 8)), (2, 1, 8, 2.0), jnp.float32),
        "other_down": noise(arg_keys[1], (EXPERTS, D_EXPERT, D_MODEL), (D_EXPERT * 4) ** -0.5, 0.0390625, ((0, 4), (2, 8))),
        "router_weight": noise(arg_keys[2], (D_MODEL, EXPERTS), D_MODEL ** -0.5, 0.09375, ((0, 8), (1, 4)), jnp.float32),
        "router_gain": jnp.clip(1.0 + 0.15 * jax.random.normal(arg_keys[3], (D_MODEL,), jnp.float32), 0.25, 1.75),
    }


def reference(train_down, other_down, router_weight, router_gain):
    latest_down = train_down + other_down.astype(jnp.float32)
    scale_down = jnp.max(jnp.abs(latest_down), axis=2)
    ready_down = (latest_down / jnp.expand_dims(scale_down, 2)).astype(jnp.bfloat16)
    serve_router = (router_weight * router_gain[:, None]).astype(jnp.bfloat16)
    return ready_down, scale_down, serve_router
```

```python
import functools

import jax
import jax.numpy as jnp
from jax import lax
from jax.experimental import pallas as pl
from jax.experimental.pallas import tpu as pltpu
from jax.sharding import PartitionSpec as P

MESH = pl.DeviceIdType.MESH
AHEAD = 3
DEPTH = 10
LANES = 128


def exchange(
    groups, shards, parts, direct,
    train, other, router, gain,
    ready, scale_out, serve,
    tbuf, obuf, stage, lmax, amax, rmax, hown, xmax, gown, gmax, rparts, rflip,
    tsem, osem, data_send, data_recv, a_send, a_recv,
    p1_send, p1_recv, p2_send, p2_recv, p3_send, p3_recv,
    r1_send, r1_recv, r2_send, r2_recv, r3_send, r3_recv,
):
    me = lax.axis_index("shard")
    group = lax.axis_index("expert")
    experts = train.shape[0]
    slots, _, rows, cols = tbuf.shape
    depth = stage.shape[0]
    chunks = experts * parts
    block = rows * parts
    half = shards // 2
    side, seat = me // half, lax.rem(me, half)

    def shard_id(k):
        return lax.rem(me + k, shards)

    def group_id(k):
        return lax.rem(group + k, groups)

    def seat_id(k):
        return lax.rem(seat + k, half)

    across = lax.rem(me + half, shards)

    barrier = pltpu.get_barrier_semaphore()
    for k in range(1, shards):
        pl.semaphore_signal(barrier, inc=1, device_id=(group, shard_id(k)), device_id_type=MESH)
    for k in range(1, groups):
        pl.semaphore_signal(barrier, inc=1, device_id=(group_id(k), me), device_id_type=MESH)

    def place(c, d):
        return c // parts, pl.ds(pl.multiple_of(d * block + lax.rem(c, parts) * rows, 8), rows)

    def load(c, d):
        e, span = place(c, d)
        slot = lax.rem(c, slots)
        return (
            pltpu.make_async_copy(train.at[e, span], tbuf.at[slot, d], tsem.at[slot, d]),
            pltpu.make_async_copy(other.at[e, span], obuf.at[slot, d], osem.at[slot, d]),
        )

    def start_load(c):
        def one(d, _):
            for copy in load(c, d):
                copy.start()
            return 0
        lax.fori_loop(0, shards, one, 0)

    def columns_of(d):
        return pl.ds(pl.multiple_of(d * cols, LANES), cols)

    def send(src, dst, send_sem, recv_sem, peer):
        return pltpu.make_async_remote_copy(
            src_ref=src, dst_ref=dst, send_sem=send_sem, recv_sem=recv_sem,
            device_id=(group, peer), device_id_type=MESH,
        )

    def wait_for(some, sem):
        pltpu.make_async_copy(some, some, sem).wait()

    def find_max(c):
        slot = lax.rem(c, slots)

        def one(d, _):
            for copy in load(c, d):
                copy.wait()
            best = None
            for j in range(0, cols, LANES):
                at = pl.ds(j, LANES)
                now = jnp.abs(tbuf[slot, d, :, at] + obuf[slot, d, :, at].astype(jnp.float32))
                best = now if best is None else jnp.maximum(best, now)
            lmax[c, d // half, lax.rem(d, half)] = jnp.max(best.T, axis=0, keepdims=True)
            return 0
        lax.fori_loop(0, shards, one, 0)

    def tell_all(c):
        def tell(k, _):
            send(lmax.at[c], amax.at[c, me], a_send.at[c], a_recv.at[c], shard_id(k)).start()
            return 0
        lax.fori_loop(1, shards, tell, 0)
        amax[c, me] = lmax[c]

    def hear_all(c):
        wait_for(amax.at[c, pl.ds(0, shards - 1)], a_recv.at[c])
        best = amax[c, 0]
        for d in range(1, shards):
            best = jnp.maximum(best, amax[c, d])
        for j in range(half):
            gmax[c, j] = best[:, j]

    def tell_leaders(c):
        def tell(k, _):
            j = seat_id(k)
            send(lmax.at[c, :, j], rmax.at[c, seat], p1_send.at[c], p1_recv.at[c], side * half + j).start()
            return 0
        lax.fori_loop(1, half, tell, 0)
        rmax[c, seat] = lmax[c, :, seat]

    def tell_across(c):
        wait_for(rmax.at[c, pl.ds(0, half - 1)], p1_recv.at[c])
        best = rmax[c, 0]
        for j in range(1, half):
            best = jnp.maximum(best, rmax[c, j])
        hown[c] = best
        send(hown.at[c], xmax.at[c], p2_send.at[c], p2_recv.at[c], across).start()

    def tell_half(c):
        wait_for(xmax.at[c], p2_recv.at[c])
        best = jnp.maximum(hown[c], xmax[c])
        gown[c] = best

        def tell(k, _):
            send(gown.at[c], gmax.at[c, seat], p3_send.at[c], p3_recv.at[c], side * half + seat_id(k)).start()
            return 0
        lax.fori_loop(1, half, tell, 0)
        gmax[c, seat] = best

    def narrow(c):
        slot = lax.rem(c, slots)
        berth = lax.rem(c, depth)
        e = c // parts
        span = pl.ds(pl.multiple_of(lax.rem(c, parts) * rows, 8), rows)

        @pl.when(c < direct)
        def _():
            hear_all(c)

        @pl.when(c >= direct)
        def _():
            wait_for(gmax.at[c, pl.ds(0, half - 1)], p3_recv.at[c])

        @pl.when(c >= depth)
        def _():
            wait_for(stage.at[berth, pl.ds(0, shards - 1)], data_send.at[berth])
        scale_out[c] = gmax[c, seat, side]

        def one(k, _):
            d = lax.rem(me + half + k, shards)
            tall = jnp.broadcast_to(gmax[c, lax.rem(d, half), d // half], (LANES, rows)).T
            for j in range(0, cols, LANES):
                at = pl.ds(j, LANES)
                now = tbuf[slot, d, :, at] + obuf[slot, d, :, at].astype(jnp.float32)
                stage[berth, d, :, at] = (now / tall).astype(jnp.bfloat16)

            @pl.when(d != me)
            def _():
                send(
                    stage.at[berth, d], ready.at[e, span, columns_of(me)],
                    data_send.at[berth], data_recv.at[me], d,
                ).start()

            @pl.when(d == me)
            def _():
                ready[e, span, columns_of(me)] = stage[berth, me]
            return 0
        lax.fori_loop(0, shards, one, 0)

    for c in range(direct):
        start_load(c)
    for c in range(direct):
        find_max(c)
    for c in range(direct, min(AHEAD + 2, chunks)):
        start_load(c)
    rparts[group, side, seat] = router[...] * gain[...]
    pl.semaphore_wait(barrier, shards - 1 + groups - 1)
    for c in range(direct):
        tell_all(c)
    mine = rparts.at[group, side, seat]
    send(mine, mine, r1_send, r1_recv, across).start()

    def step(c, _):
        @pl.when(c < chunks)
        def _():
            find_max(c)
            tell_leaders(c)

        @pl.when((c >= direct + 1) & (c <= chunks))
        def _():
            tell_across(c - 1)

        @pl.when((c >= direct + 2) & (c <= chunks + 1))
        def _():
            tell_half(c - 2)

        @pl.when(c == AHEAD)
        def _():
            wait_for(mine, r1_recv)
            for k in range(1, half):
                both = rparts.at[group, :, seat]
                send(both, both, r2_send, r2_recv, side * half + seat_id(k)).start()

        @pl.when(c == min(AHEAD + 1, chunks + AHEAD - 1))
        def _():
            wait_for(rparts.at[group, :, pl.ds(0, half - 1)], r2_recv)
            for k in range(1, groups):
                pltpu.make_async_remote_copy(
                    src_ref=rparts.at[group], dst_ref=rparts.at[group], send_sem=r3_send, recv_sem=r3_recv,
                    device_id=(group_id(k), me), device_id_type=MESH,
                ).start()

        narrow(c - AHEAD)

        @pl.when(c + 2 < chunks)
        def _():
            start_load(c + 2)
        return 0

    lax.fori_loop(AHEAD, chunks + AHEAD, step, 0)

    wait_for(rparts.at[pl.ds(0, groups - 1)], r3_recv)
    wide = router.shape[1]
    for d in range(shards):
        for g in range(groups):
            rflip[g * experts:(g + 1) * experts, :] = rparts[g, d // half, d % half]
        serve[:, d * wide:(d + 1) * wide] = rflip[...].astype(jnp.bfloat16)

    wait_for(mine, r1_send)
    wait_for(rparts.at[group, :, pl.ds(0, half - 1)], r2_send)
    wait_for(rparts.at[pl.ds(0, groups - 1)], r3_send)
    for c in range(direct):
        wait_for(amax.at[c, pl.ds(0, shards - 1)], a_send.at[c])

    def drain(c, _):
        wait_for(rmax.at[c, pl.ds(0, half - 1)], p1_send.at[c])
        wait_for(xmax.at[c], p2_send.at[c])
        wait_for(gmax.at[c, pl.ds(0, half - 1)], p3_send.at[c])
        return 0
    lax.fori_loop(direct, chunks, drain, 0)

    def unload(berth, _):
        wait_for(stage.at[berth, pl.ds(0, shards - 1)], data_send.at[berth])
        return 0
    lax.fori_loop(0, min(depth, chunks), unload, 0)

    def finish(k, _):
        d = shard_id(k)
        wait_for(ready.at[:, :, columns_of(d)], data_recv.at[d])
        return 0
    lax.fori_loop(1, shards, finish, 0)


def write_out(parts, landed, scale_in, serve_in, ready, scale, serve, sem):
    experts, block, _ = landed.shape
    rows = block // parts
    for e in range(experts):
        for p in range(parts):
            span = pl.ds(p * rows, rows)
            pltpu.make_async_copy(landed.at[e, span], ready.at[e, span], sem).start()
    serve[...] = serve_in[...]
    for e in range(experts):
        scale[e:e + 1, :] = jnp.concatenate([scale_in[e * parts + p] for p in range(parts)], axis=1)
    pltpu.make_async_copy(landed, ready, sem).wait()


def pieces(block):
    for count in (5, 4, 3, 2):
        if block % (16 * count) == 0:
            return count
    return 1


def per_device(groups, shards, train_down, other_down, router_weight, router_gain):
    experts, height, cols = train_down.shape
    block = height // shards
    parts = pieces(block)
    rows = block // parts
    chunks = experts * parts
    direct = min(AHEAD, chunks)
    slots = AHEAD + 2
    depth = min(DEPTH, chunks)
    half = shards // 2
    wide = router_weight.shape[0]
    f32, bf16 = jnp.float32, jnp.bfloat16
    dma = pltpu.SemaphoreType.DMA
    hbm = pl.BlockSpec(memory_space=pl.ANY)
    vmem = pl.BlockSpec(memory_space=pltpu.VMEM)
    landed, scale, serve = pl.pallas_call(
        functools.partial(exchange, groups, shards, parts, direct),
        out_shape=(
            pltpu.VMEM((experts, block, cols * shards), bf16),
            pltpu.VMEM((chunks, 1, rows), f32),
            pltpu.VMEM((experts * groups, wide * shards), bf16),
        ),
        in_specs=[hbm, hbm, vmem, vmem],
        out_specs=(vmem, vmem, vmem),
        scratch_shapes=[
            pltpu.VMEM((slots, shards, rows, cols), f32),
            pltpu.VMEM((slots, shards, rows, cols), bf16),
            pltpu.VMEM((depth, shards, rows, cols), bf16),
            pltpu.VMEM((chunks, 2, half, 1, rows), f32),
            pltpu.VMEM((direct, shards, 2, half, 1, rows), f32),
            pltpu.VMEM((chunks, half, 2, 1, rows), f32),
            pltpu.VMEM((chunks, 2, 1, rows), f32),
            pltpu.VMEM((chunks, 2, 1, rows), f32),
            pltpu.VMEM((chunks, 2, 1, rows), f32),
            pltpu.VMEM((chunks, half, 2, 1, rows), f32),
            pltpu.VMEM((groups, 2, half, experts, wide), f32),
            pltpu.VMEM((groups * experts, wide), f32),
            dma((slots, shards)), dma((slots, shards)),
            dma((depth,)), dma((shards,)),
            dma((direct,)), dma((direct,)),
            dma((chunks,)), dma((chunks,)), dma((chunks,)), dma((chunks,)), dma((chunks,)), dma((chunks,)),
            dma(()), dma(()), dma(()), dma(()), dma(()), dma(()),
        ],
        compiler_params=pltpu.CompilerParams(
            collective_id=0, has_side_effects=True, vmem_limit_bytes=36 * 2**20
        ),
    )(train_down, other_down, router_weight.T, router_gain[None, :])
    ready, scale, serve = pl.pallas_call(
        functools.partial(write_out, parts),
        out_shape=(
            jax.ShapeDtypeStruct((experts, block, cols * shards), bf16),
            jax.ShapeDtypeStruct((experts, block), f32),
            jax.ShapeDtypeStruct((experts * groups, wide * shards), bf16),
        ),
        in_specs=[vmem, vmem, vmem],
        out_specs=(hbm, vmem, vmem),
        scratch_shapes=[dma(())],
        compiler_params=pltpu.CompilerParams(vmem_limit_bytes=8 * 2**20),
    )(landed, scale, serve)
    return ready, scale, serve.T


def solution(mesh):
    in_specs = (
        P("expert", None, "shard"),
        P("expert", None, "shard"),
        P("shard", "expert"),
        P("shard"),
    )
    out_specs = (P("expert", "shard", None), P("expert", "shard"), P())
    body = functools.partial(per_device, mesh.shape["expert"], mesh.shape["shard"])
    return jax.shard_map(
        body, mesh=mesh, in_specs=in_specs, out_specs=out_specs, check_vma=False
    )
```

```python
import functools

import jax
import jax.numpy as jnp
from jax import lax
from jax.experimental import pallas as pl
from jax.experimental.pallas import tpu as pltpu
from jax.sharding import PartitionSpec as P

MESH = pl.DeviceIdType.MESH
AHEAD = 3
DEPTH = 10
LATE = 192
LANES = 128


def exchange(
    groups, shards, parts, direct, late,
    train, other, router, gain,
    ready, scale_out, serve, last,
    tbuf, obuf, stage, lmax, amax, rmax, hown, xmax, gown, gmax, rparts, rflip,
    tsem, osem, data_send, data_recv, a_send, a_recv,
    p1_send, p1_recv, p2_send, p2_recv, p3_send, p3_recv,
    r1_send, r1_recv, r2_send, r2_recv, r3_send, r3_recv,
):
    me = lax.axis_index("shard")
    group = lax.axis_index("expert")
    experts = train.shape[0]
    slots, _, rows, cols = tbuf.shape
    depth = stage.shape[0]
    total = experts * parts * rows
    chunks = experts * parts
    block = rows * parts
    half = shards // 2
    side, seat = me // half, lax.rem(me, half)

    def shard_id(k):
        return lax.rem(me + k, shards)

    def group_id(k):
        return lax.rem(group + k, groups)

    def seat_id(k):
        return lax.rem(seat + k, half)

    across = lax.rem(me + half, shards)
    kept = {}
    for c in range(chunks - 1, -1, -1):
        left = max(0, min(rows, total - late - c * rows))
        if left < rows:
            kept[c] = left

    def held(c, b):
        if c in kept:
            return stage.at[b, pl.ds(0, (shards - 2) * rows + kept[c])]
        return stage.at[b, pl.ds(0, (shards - 1) * rows)]

    barrier = pltpu.get_barrier_semaphore()
    for k in range(1, shards):
        pl.semaphore_signal(barrier, inc=1, device_id=(group, shard_id(k)), device_id_type=MESH)
    for k in range(1, groups):
        pl.semaphore_signal(barrier, inc=1, device_id=(group_id(k), me), device_id_type=MESH)

    def place(c, d):
        return c // parts, pl.ds(pl.multiple_of(d * block + lax.rem(c, parts) * rows, 8), rows)

    def load(c, d):
        e, span = place(c, d)
        slot = lax.rem(c, slots)
        return (
            pltpu.make_async_copy(train.at[e, span], tbuf.at[slot, d], tsem.at[slot, d]),
            pltpu.make_async_copy(other.at[e, span], obuf.at[slot, d], osem.at[slot, d]),
        )

    def start_load(c):
        def one(d, _):
            for copy in load(c, d):
                copy.start()
            return 0
        lax.fori_loop(0, shards, one, 0)

    def columns_of(d):
        return pl.ds(pl.multiple_of(d * cols, LANES), cols)

    def send(src, dst, send_sem, recv_sem, peer):
        return pltpu.make_async_remote_copy(
            src_ref=src, dst_ref=dst, send_sem=send_sem, recv_sem=recv_sem,
            device_id=(group, peer), device_id_type=MESH,
        )

    def wait_for(some, sem):
        pltpu.make_async_copy(some, some, sem).wait()

    def find_max(c):
        slot = lax.rem(c, slots)

        def one(d, _):
            for copy in load(c, d):
                copy.wait()
            best = None
            for j in range(0, cols, LANES):
                at = pl.ds(j, LANES)
                now = jnp.abs(tbuf[slot, d, :, at] + obuf[slot, d, :, at].astype(jnp.float32))
                best = now if best is None else jnp.maximum(best, now)
            lmax[c, d // half, lax.rem(d, half)] = jnp.max(best.T, axis=0, keepdims=True)
            return 0
        lax.fori_loop(0, shards, one, 0)

    def tell_all(c):
        def tell(k, _):
            send(lmax.at[c], amax.at[c, me], a_send.at[c], a_recv.at[c], shard_id(k)).start()
            return 0
        lax.fori_loop(1, shards, tell, 0)
        amax[c, me] = lmax[c]

    def hear_all(c):
        wait_for(amax.at[c, pl.ds(0, shards - 1)], a_recv.at[c])
        best = amax[c, 0]
        for d in range(1, shards):
            best = jnp.maximum(best, amax[c, d])
        for j in range(half):
            gmax[c, j] = best[:, j]

    def tell_leaders(c):
        def tell(k, _):
            j = seat_id(k)
            send(lmax.at[c, :, j], rmax.at[c, seat], p1_send.at[c], p1_recv.at[c], side * half + j).start()
            return 0
        lax.fori_loop(1, half, tell, 0)
        rmax[c, seat] = lmax[c, :, seat]

    def tell_across(c):
        wait_for(rmax.at[c, pl.ds(0, half - 1)], p1_recv.at[c])
        best = rmax[c, 0]
        for j in range(1, half):
            best = jnp.maximum(best, rmax[c, j])
        hown[c] = best
        send(hown.at[c], xmax.at[c], p2_send.at[c], p2_recv.at[c], across).start()

    def tell_half(c):
        wait_for(xmax.at[c], p2_recv.at[c])
        best = jnp.maximum(hown[c], xmax[c])
        gown[c] = best

        def tell(k, _):
            send(gown.at[c], gmax.at[c, seat], p3_send.at[c], p3_recv.at[c], side * half + seat_id(k)).start()
            return 0
        lax.fori_loop(1, half, tell, 0)
        gmax[c, seat] = best

    def narrow(c):
        slot = lax.rem(c, slots)
        berth = lax.rem(c, depth)
        first = pl.multiple_of(c * rows, 8)

        @pl.when(c < direct)
        def _():
            hear_all(c)

        @pl.when(c >= direct)
        def _():
            wait_for(gmax.at[c, pl.ds(0, half - 1)], p3_recv.at[c])

        @pl.when(c >= depth)
        def _():
            wait_for(held(None, berth), data_send.at[berth])
        scale_out[c] = gmax[c, seat, side]

        def one(k, _):
            d = lax.rem(me + half + k, shards)
            tall = jnp.broadcast_to(gmax[c, lax.rem(d, half), d // half], (LANES, rows)).T
            for j in range(0, cols, LANES):
                at = pl.ds(j, LANES)
                now = tbuf[slot, d, :, at] + obuf[slot, d, :, at].astype(jnp.float32)
                stage[berth, pl.ds(pl.multiple_of(d * rows, 8), rows), at] = (now / tall).astype(jnp.bfloat16)

            def part(count):
                send(
                    stage.at[berth, pl.ds(pl.multiple_of(d * rows, 8), count)],
                    ready.at[pl.ds(first, count), columns_of(me)],
                    data_send.at[berth], data_recv.at[me], d,
                ).start()

            whole = d != me
            for special in kept:
                whole = whole & ((k > 0) | (c != special))

            @pl.when(whole)
            def _():
                part(rows)

            for special, left in kept.items():
                @pl.when((k == 0) & (c == special))
                def _():
                    if left:
                        part(left)
                    at = special * rows + left - (total - late)
                    last[at:at + rows - left, :] = stage[berth, pl.ds(pl.multiple_of(d * rows + left, 8), rows - left), :]

            @pl.when(d == me)
            def _():
                ready[pl.ds(first, rows), columns_of(me)] = stage[berth, pl.ds(pl.multiple_of(d * rows, 8), rows), :]
            return 0
        lax.fori_loop(0, shards, one, 0)

    for c in range(direct):
        start_load(c)
    for c in range(direct):
        find_max(c)
    for c in range(direct, min(AHEAD + 2, chunks)):
        start_load(c)
    rparts[group, side, seat] = router[...] * gain[...]
    pl.semaphore_wait(barrier, shards - 1 + groups - 1)
    for c in range(direct):
        tell_all(c)
    mine = rparts.at[group, side, seat]
    send(mine, mine, r1_send, r1_recv, across).start()

    def step(c, _):
        @pl.when(c < chunks)
        def _():
            find_max(c)
            tell_leaders(c)

        @pl.when((c >= direct + 1) & (c <= chunks))
        def _():
            tell_across(c - 1)

        @pl.when((c >= direct + 2) & (c <= chunks + 1))
        def _():
            tell_half(c - 2)

        @pl.when(c == AHEAD)
        def _():
            wait_for(mine, r1_recv)
            for k in range(1, half):
                both = rparts.at[group, :, seat]
                send(both, both, r2_send, r2_recv, side * half + seat_id(k)).start()

        @pl.when(c == min(AHEAD + 1, chunks + AHEAD - 1))
        def _():
            wait_for(rparts.at[group, :, pl.ds(0, half - 1)], r2_recv)
            for k in range(1, groups):
                pltpu.make_async_remote_copy(
                    src_ref=rparts.at[group], dst_ref=rparts.at[group], send_sem=r3_send, recv_sem=r3_recv,
                    device_id=(group_id(k), me), device_id_type=MESH,
                ).start()

        narrow(c - AHEAD)

        @pl.when(c + 2 < chunks)
        def _():
            start_load(c + 2)
        return 0

    lax.fori_loop(AHEAD, chunks + AHEAD, step, 0)

    wait_for(rparts.at[pl.ds(0, groups - 1)], r3_recv)
    wide = router.shape[1]
    for d in range(shards):
        for g in range(groups):
            rflip[g * experts:(g + 1) * experts, :] = rparts[g, d // half, d % half]
        serve[:, d * wide:(d + 1) * wide] = rflip[...].astype(jnp.bfloat16)

    wait_for(mine, r1_send)
    wait_for(rparts.at[group, :, pl.ds(0, half - 1)], r2_send)
    wait_for(rparts.at[pl.ds(0, groups - 1)], r3_send)
    for c in range(direct):
        wait_for(amax.at[c, pl.ds(0, shards - 1)], a_send.at[c])

    def drain(c, _):
        wait_for(rmax.at[c, pl.ds(0, half - 1)], p1_send.at[c])
        wait_for(xmax.at[c], p2_send.at[c])
        wait_for(gmax.at[c, pl.ds(0, half - 1)], p3_send.at[c])
        return 0
    lax.fori_loop(direct, chunks, drain, 0)

    for c in range(chunks - depth, chunks):
        wait_for(held(c, c % depth), data_send.at[c % depth])

    wait_for(ready.at[pl.ds(0, total - late), columns_of(across)], data_recv.at[across])

    def finish(k, _):
        d = lax.rem(across + k, shards)

        @pl.when(d != me)
        def _():
            wait_for(ready.at[:, columns_of(d)], data_recv.at[d])
        return 0
    lax.fori_loop(1, shards, finish, 0)


def write_out(parts, landed, scale_in, serve_in, ready, scale, serve, rows_of, sem, scale_sem, serve_sem):
    experts, block, _ = ready.shape
    rows = block // parts
    for e in range(experts):
        pltpu.make_async_copy(landed.at[pl.ds(e * block, block)], ready.at[e], sem.at[e]).start()
    pltpu.make_async_copy(serve_in, serve, serve_sem).start()
    for e in range(experts):
        rows_of[e:e + 1, :] = jnp.concatenate([scale_in[e * parts + p] for p in range(parts)], axis=1)
    pltpu.make_async_copy(rows_of, scale, scale_sem).start()
    pltpu.make_async_copy(serve_in, serve, serve_sem).wait()
    pltpu.make_async_copy(rows_of, scale, scale_sem).wait()
    for e in range(experts):
        pltpu.make_async_copy(landed.at[pl.ds(e * block, block)], ready.at[e], sem.at[e]).wait()


def add_last(shards, ready_in, last, ready, sem):
    late, cols = last.shape
    experts, block, _ = ready.shape
    across = lax.rem(lax.axis_index("shard") + shards // 2, shards)
    copy = pltpu.make_async_copy(
        last, ready.at[experts - 1, pl.ds(block - late, late), pl.ds(pl.multiple_of(across * cols, LANES), cols)], sem
    )
    copy.start()
    copy.wait()


def pieces(block):
    for count in (5, 4, 3, 2):
        if block % (16 * count) == 0:
            return count
    return 1


def per_device(groups, shards, train_down, other_down, router_weight, router_gain):
    experts, height, cols = train_down.shape
    block = height // shards
    parts = pieces(block)
    rows = block // parts
    chunks = experts * parts
    direct = min(AHEAD, chunks)
    slots = AHEAD + 2
    depth = min(DEPTH, chunks)
    half = shards // 2
    wide = router_weight.shape[0]
    late = LATE if chunks > depth and LATE < block else 0
    f32, bf16 = jnp.float32, jnp.bfloat16
    dma = pltpu.SemaphoreType.DMA
    hbm = pl.BlockSpec(memory_space=pl.ANY)
    vmem = pl.BlockSpec(memory_space=pltpu.VMEM)
    landed, scale, serve, last = pl.pallas_call(
        functools.partial(exchange, groups, shards, parts, direct, late),
        out_shape=(
            pltpu.VMEM((experts * block, cols * shards), bf16),
            pltpu.VMEM((chunks, 1, rows), f32),
            pltpu.VMEM((experts * groups, wide * shards), bf16),
            pltpu.VMEM((max(late, 16), cols), bf16),
        ),
        in_specs=[hbm, hbm, vmem, vmem],
        out_specs=(vmem, vmem, vmem, vmem),
        scratch_shapes=[
            pltpu.VMEM((slots, shards, rows, cols), f32),
            pltpu.VMEM((slots, shards, rows, cols), bf16),
            pltpu.VMEM((depth, shards * rows, cols), bf16),
            pltpu.VMEM((chunks, 2, half, 1, rows), f32),
            pltpu.VMEM((direct, shards, 2, half, 1, rows), f32),
            pltpu.VMEM((chunks, half, 2, 1, rows), f32),
            pltpu.VMEM((chunks, 2, 1, rows), f32),
            pltpu.VMEM((chunks, 2, 1, rows), f32),
            pltpu.VMEM((chunks, 2, 1, rows), f32),
            pltpu.VMEM((chunks, half, 2, 1, rows), f32),
            pltpu.VMEM((groups, 2, half, experts, wide), f32),
            pltpu.VMEM((groups * experts, wide), f32),
            dma((slots, shards)), dma((slots, shards)),
            dma((depth,)), dma((shards,)),
            dma((direct,)), dma((direct,)),
            dma((chunks,)), dma((chunks,)), dma((chunks,)), dma((chunks,)), dma((chunks,)), dma((chunks,)),
            dma(()), dma(()), dma(()), dma(()), dma(()), dma(()),
        ],
        compiler_params=pltpu.CompilerParams(
            collective_id=0, has_side_effects=True, vmem_limit_bytes=36 * 2**20
        ),
    )(train_down, other_down, router_weight.T, router_gain[None, :])
    if late:
        swap = [(d, (d + half) % shards) for d in range(shards)]
        last = lax.ppermute(last, "shard", swap)
    ready, scale, serve = pl.pallas_call(
        functools.partial(write_out, parts),
        out_shape=(
            jax.ShapeDtypeStruct((experts, block, cols * shards), bf16),
            jax.ShapeDtypeStruct((experts, block), f32),
            jax.ShapeDtypeStruct((experts * groups, wide * shards), bf16),
        ),
        in_specs=[vmem, vmem, vmem],
        out_specs=(hbm, hbm, hbm),
        scratch_shapes=[pltpu.VMEM((experts, block), f32), dma((experts,)), dma(()), dma(())],
        cost_estimate=pl.CostEstimate(flops=0, bytes_accessed=4 * experts * block * cols * shards, transcendentals=0),
        compiler_params=pltpu.CompilerParams(vmem_limit_bytes=4 * 2**20),
    )(landed, scale, serve)
    if late:
        ready = pl.pallas_call(
            functools.partial(add_last, shards),
            out_shape=jax.ShapeDtypeStruct(ready.shape, bf16),
            in_specs=[hbm, vmem],
            out_specs=hbm,
            input_output_aliases={0: 0},
            scratch_shapes=[dma(())],
            compiler_params=pltpu.CompilerParams(vmem_limit_bytes=4 * 2**20),
        )(ready, last)
    return ready, scale, serve.T


def solution(mesh):
    in_specs = (
        P("expert", None, "shard"),
        P("expert", None, "shard"),
        P("shard", "expert"),
        P("shard"),
    )
    out_specs = (P("expert", "shard", None), P("expert", "shard"), P())
    body = functools.partial(per_device, mesh.shape["expert"], mesh.shape["shard"])
    return jax.shard_map(
        body, mesh=mesh, in_specs=in_specs, out_specs=out_specs, check_vma=False
    )
```

```python
import functools

import jax
import jax.numpy as jnp
from jax import lax
from jax.experimental import pallas as pl
from jax.experimental.pallas import tpu as pltpu
from jax.sharding import PartitionSpec as P

MESH = pl.DeviceIdType.MESH
AHEAD = 3
DEPTH = 10
SOON = 2
EARLY = 2
LATE = 192
LANES = 128


def exchange(
    groups, shards, parts, direct, late,
    train, other, router, gain,
    ready, scale_out, serve, last,
    tbuf, obuf, stage, lmax, amax, rmax, hown, xmax, gown, gmax, rparts, rflip,
    tsem, osem, data_send, data_recv, a_send, a_recv,
    p1_send, p1_recv, p2_send, p2_recv, p3_send, p3_recv,
    r1_send, r1_recv, r2_send, r2_recv, r3_send, r3_recv,
):
    me = lax.axis_index("shard")
    group = lax.axis_index("expert")
    experts = train.shape[0]
    slots, _, rows, cols = tbuf.shape
    depth = stage.shape[0]
    total = experts * parts * rows
    chunks = experts * parts
    block = rows * parts
    half = shards // 2
    side, seat = me // half, lax.rem(me, half)

    def shard_id(k):
        return lax.rem(me + k, shards)

    def group_id(k):
        return lax.rem(group + k, groups)

    def seat_id(k):
        return lax.rem(seat + k, half)

    across = lax.rem(me + half, shards)
    kept = {}
    for c in range(chunks - 1, -1, -1):
        left = max(0, min(rows, total - late - c * rows))
        if left < rows:
            kept[c] = left

    def held(c, b):
        if c in kept:
            return stage.at[b, pl.ds(0, (shards - 2) * rows + kept[c])]
        return stage.at[b, pl.ds(0, (shards - 1) * rows)]

    barrier = pltpu.get_barrier_semaphore()
    for k in range(1, shards):
        pl.semaphore_signal(barrier, inc=1, device_id=(group, shard_id(k)), device_id_type=MESH)
    for k in range(1, groups):
        pl.semaphore_signal(barrier, inc=1, device_id=(group_id(k), me), device_id_type=MESH)

    def place(c, d):
        return c // parts, pl.ds(pl.multiple_of(d * block + lax.rem(c, parts) * rows, 8), rows)

    def load(c, d):
        e, span = place(c, d)
        slot = lax.rem(c, slots)
        return (
            pltpu.make_async_copy(train.at[e, span], tbuf.at[slot, d], tsem.at[slot, d]),
            pltpu.make_async_copy(other.at[e, span], obuf.at[slot, d], osem.at[slot, d]),
        )

    def start_load(c):
        def one(d, _):
            for copy in load(c, d):
                copy.start()
            return 0
        lax.fori_loop(0, shards, one, 0)

    def columns_of(d):
        return pl.ds(pl.multiple_of(d * cols, LANES), cols)

    def send(src, dst, send_sem, recv_sem, peer):
        return pltpu.make_async_remote_copy(
            src_ref=src, dst_ref=dst, send_sem=send_sem, recv_sem=recv_sem,
            device_id=(group, peer), device_id_type=MESH,
        )

    def wait_for(some, sem):
        pltpu.make_async_copy(some, some, sem).wait()

    def find_max(c):
        slot = lax.rem(c, slots)

        def one(d, _):
            for copy in load(c, d):
                copy.wait()
            best = None
            for j in range(0, cols, LANES):
                at = pl.ds(j, LANES)
                now = jnp.abs(tbuf[slot, d, :, at] + obuf[slot, d, :, at].astype(jnp.float32))
                best = now if best is None else jnp.maximum(best, now)
            lmax[c, d // half, lax.rem(d, half)] = jnp.max(best.T, axis=0, keepdims=True)
            return 0
        lax.fori_loop(0, shards, one, 0)

    def tell_all(c):
        def tell(k, _):
            send(lmax.at[c], amax.at[c, me], a_send.at[c], a_recv.at[c], shard_id(k)).start()
            return 0
        lax.fori_loop(1, shards, tell, 0)
        amax[c, me] = lmax[c]

    def hear_all(c):
        wait_for(amax.at[c, pl.ds(0, shards - 1)], a_recv.at[c])
        best = amax[c, 0]
        for d in range(1, shards):
            best = jnp.maximum(best, amax[c, d])
        for j in range(half):
            gmax[c, j] = best[:, j]

    def tell_leaders(c):
        def tell(k, _):
            j = seat_id(k)
            send(lmax.at[c, :, j], rmax.at[c, seat], p1_send.at[c], p1_recv.at[c], side * half + j).start()
            return 0
        lax.fori_loop(1, half, tell, 0)
        rmax[c, seat] = lmax[c, :, seat]

    def tell_across(c):
        wait_for(rmax.at[c, pl.ds(0, half - 1)], p1_recv.at[c])
        best = rmax[c, 0]
        for j in range(1, half):
            best = jnp.maximum(best, rmax[c, j])
        hown[c] = best
        send(hown.at[c], xmax.at[c], p2_send.at[c], p2_recv.at[c], across).start()

    def tell_half(c):
        wait_for(xmax.at[c], p2_recv.at[c])
        best = jnp.maximum(hown[c], xmax[c])
        gown[c] = best

        def tell(k, _):
            send(gown.at[c], gmax.at[c, seat], p3_send.at[c], p3_recv.at[c], side * half + seat_id(k)).start()
            return 0
        lax.fori_loop(1, half, tell, 0)
        gmax[c, seat] = best

    def open_chunk(c):
        berth = lax.rem(c, depth)

        @pl.when(c < direct)
        def _():
            hear_all(c)

        @pl.when(c >= direct)
        def _():
            wait_for(gmax.at[c, pl.ds(0, half - 1)], p3_recv.at[c])

        @pl.when(c >= depth)
        def _():
            wait_for(held(None, berth), data_send.at[berth])
        scale_out[c] = gmax[c, seat, side]

    def narrow(c, begin, end):
        slot = lax.rem(c, slots)
        berth = lax.rem(c, depth)
        first = pl.multiple_of(c * rows, 8)

        def one(k, _):
            d = lax.rem(me + half + half * lax.rem(c, 2) + k, shards)
            tall = jnp.broadcast_to(gmax[c, lax.rem(d, half), d // half], (LANES, rows)).T
            for j in range(0, cols, LANES):
                at = pl.ds(j, LANES)
                now = tbuf[slot, d, :, at] + obuf[slot, d, :, at].astype(jnp.float32)
                stage[berth, pl.ds(pl.multiple_of(d * rows, 8), rows), at] = (now / tall).astype(jnp.bfloat16)

            def part(count):
                send(
                    stage.at[berth, pl.ds(pl.multiple_of(d * rows, 8), count)],
                    ready.at[pl.ds(first, count), columns_of(me)],
                    data_send.at[berth], data_recv.at[me], d,
                ).start()

            whole = d != me
            for special in kept:
                whole = whole & ((d != across) | (c != special))

            @pl.when(whole)
            def _():
                part(rows)

            for special, left in kept.items():
                @pl.when((d == across) & (c == special))
                def _():
                    if left:
                        part(left)
                    at = special * rows + left - (total - late)
                    last[at:at + rows - left, :] = stage[berth, pl.ds(pl.multiple_of(d * rows + left, 8), rows - left), :]

            @pl.when(d == me)
            def _():
                ready[pl.ds(first, rows), columns_of(me)] = stage[berth, pl.ds(pl.multiple_of(d * rows, 8), rows), :]
            return 0
        lax.fori_loop(begin, end, one, 0)

    for c in range(direct):
        start_load(c)
    for c in range(min(SOON, direct)):
        find_max(c)
    for c in range(direct, min(AHEAD + 2, chunks)):
        start_load(c)
    rparts[group, side, seat] = router[...] * gain[...]
    pl.semaphore_wait(barrier, shards - 1 + groups - 1)
    for c in range(direct):
        if c >= SOON:
            find_max(c)
        tell_all(c)
    mine = rparts.at[group, side, seat]
    send(mine, mine, r1_send, r1_recv, across).start()
    open_chunk(0)
    narrow(0, 0, EARLY)

    def step(c, _):
        @pl.when(c < chunks)
        def _():
            find_max(c)
            tell_leaders(c)

        @pl.when((c >= direct + 1) & (c <= chunks))
        def _():
            tell_across(c - 1)

        @pl.when((c >= direct + 2) & (c <= chunks + 1))
        def _():
            tell_half(c - 2)

        @pl.when(c == AHEAD)
        def _():
            wait_for(mine, r1_recv)
            for k in range(1, half):
                both = rparts.at[group, :, seat]
                send(both, both, r2_send, r2_recv, side * half + seat_id(k)).start()

        @pl.when(c == min(AHEAD + 1, chunks + AHEAD - 1))
        def _():
            wait_for(rparts.at[group, :, pl.ds(0, half - 1)], r2_recv)
            for k in range(1, groups):
                pltpu.make_async_remote_copy(
                    src_ref=rparts.at[group], dst_ref=rparts.at[group], send_sem=r3_send, recv_sem=r3_recv,
                    device_id=(group_id(k), me), device_id_type=MESH,
                ).start()

        @pl.when(c > AHEAD)
        def _():
            open_chunk(c - AHEAD)
        narrow(c - AHEAD, jnp.where(c == AHEAD, EARLY, 0), shards)

        @pl.when(c + 2 < chunks)
        def _():
            start_load(c + 2)
        return 0

    lax.fori_loop(AHEAD, chunks + AHEAD, step, 0)

    wait_for(rparts.at[pl.ds(0, groups - 1)], r3_recv)
    wide = router.shape[1]
    for d in range(shards):
        for g in range(groups):
            rflip[g * experts:(g + 1) * experts, :] = rparts[g, d // half, d % half]
        serve[:, d * wide:(d + 1) * wide] = rflip[...].astype(jnp.bfloat16)

    wait_for(mine, r1_send)
    wait_for(rparts.at[group, :, pl.ds(0, half - 1)], r2_send)
    wait_for(rparts.at[pl.ds(0, groups - 1)], r3_send)
    for c in range(direct):
        wait_for(amax.at[c, pl.ds(0, shards - 1)], a_send.at[c])

    def drain(c, _):
        wait_for(rmax.at[c, pl.ds(0, half - 1)], p1_send.at[c])
        wait_for(xmax.at[c], p2_send.at[c])
        wait_for(gmax.at[c, pl.ds(0, half - 1)], p3_send.at[c])
        return 0
    lax.fori_loop(direct, chunks, drain, 0)

    for c in range(chunks - depth, chunks):
        wait_for(held(c, c % depth), data_send.at[c % depth])

    wait_for(ready.at[pl.ds(0, total - late), columns_of(across)], data_recv.at[across])

    def finish(k, _):
        d = lax.rem(across + k, shards)

        @pl.when(d != me)
        def _():
            wait_for(ready.at[:, columns_of(d)], data_recv.at[d])
        return 0
    lax.fori_loop(1, shards, finish, 0)


def write_out(parts, landed, scale_in, serve_in, ready, scale, serve, rows_of, sem, scale_sem, serve_sem):
    experts, block, _ = ready.shape
    rows = block // parts
    for e in range(experts):
        pltpu.make_async_copy(landed.at[pl.ds(e * block, block)], ready.at[e], sem.at[e]).start()
    pltpu.make_async_copy(serve_in, serve, serve_sem).start()
    for e in range(experts):
        rows_of[e:e + 1, :] = jnp.concatenate([scale_in[e * parts + p] for p in range(parts)], axis=1)
    pltpu.make_async_copy(rows_of, scale, scale_sem).start()
    pltpu.make_async_copy(serve_in, serve, serve_sem).wait()
    pltpu.make_async_copy(rows_of, scale, scale_sem).wait()
    for e in range(experts):
        pltpu.make_async_copy(landed.at[pl.ds(e * block, block)], ready.at[e], sem.at[e]).wait()


def add_last(shards, ready_in, last, ready, sem):
    late, cols = last.shape
    experts, block, _ = ready.shape
    across = lax.rem(lax.axis_index("shard") + shards // 2, shards)
    copy = pltpu.make_async_copy(
        last, ready.at[experts - 1, pl.ds(block - late, late), pl.ds(pl.multiple_of(across * cols, LANES), cols)], sem
    )
    copy.start()
    copy.wait()


def pieces(block):
    for count in (5, 4, 3, 2):
        if block % (16 * count) == 0:
            return count
    return 1


def per_device(groups, shards, train_down, other_down, router_weight, router_gain):
    experts, height, cols = train_down.shape
    block = height // shards
    parts = pieces(block)
    rows = block // parts
    chunks = experts * parts
    direct = min(AHEAD, chunks)
    slots = AHEAD + 2
    depth = min(DEPTH, chunks)
    half = shards // 2
    wide = router_weight.shape[0]
    late = LATE if chunks > depth and LATE < block else 0
    f32, bf16 = jnp.float32, jnp.bfloat16
    dma = pltpu.SemaphoreType.DMA
    hbm = pl.BlockSpec(memory_space=pl.ANY)
    vmem = pl.BlockSpec(memory_space=pltpu.VMEM)
    landed, scale, serve, last = pl.pallas_call(
        functools.partial(exchange, groups, shards, parts, direct, late),
        out_shape=(
            pltpu.VMEM((experts * block, cols * shards), bf16),
            pltpu.VMEM((chunks, 1, rows), f32),
            pltpu.VMEM((experts * groups, wide * shards), bf16),
            pltpu.VMEM((max(late, 16), cols), bf16),
        ),
        in_specs=[hbm, hbm, vmem, vmem],
        out_specs=(vmem, vmem, vmem, vmem),
        scratch_shapes=[
            pltpu.VMEM((slots, shards, rows, cols), f32),
            pltpu.VMEM((slots, shards, rows, cols), bf16),
            pltpu.VMEM((depth, shards * rows, cols), bf16),
            pltpu.VMEM((chunks, 2, half, 1, rows), f32),
            pltpu.VMEM((direct, shards, 2, half, 1, rows), f32),
            pltpu.VMEM((chunks, half, 2, 1, rows), f32),
            pltpu.VMEM((chunks, 2, 1, rows), f32),
            pltpu.VMEM((chunks, 2, 1, rows), f32),
            pltpu.VMEM((chunks, 2, 1, rows), f32),
            pltpu.VMEM((chunks, half, 2, 1, rows), f32),
            pltpu.VMEM((groups, 2, half, experts, wide), f32),
            pltpu.VMEM((groups * experts, wide), f32),
            dma((slots, shards)), dma((slots, shards)),
            dma((depth,)), dma((shards,)),
            dma((direct,)), dma((direct,)),
            dma((chunks,)), dma((chunks,)), dma((chunks,)), dma((chunks,)), dma((chunks,)), dma((chunks,)),
            dma(()), dma(()), dma(()), dma(()), dma(()), dma(()),
        ],
        compiler_params=pltpu.CompilerParams(
            collective_id=0, has_side_effects=True, vmem_limit_bytes=36 * 2**20
        ),
    )(train_down, other_down, router_weight.T, router_gain[None, :])
    if late:
        swap = [(d, (d + half) % shards) for d in range(shards)]
        last = lax.ppermute(last, "shard", swap)
    ready, scale, serve = pl.pallas_call(
        functools.partial(write_out, parts),
        out_shape=(
            jax.ShapeDtypeStruct((experts, block, cols * shards), bf16),
            jax.ShapeDtypeStruct((experts, block), f32),
            jax.ShapeDtypeStruct((experts * groups, wide * shards), bf16),
        ),
        in_specs=[vmem, vmem, vmem],
        out_specs=(hbm, hbm, hbm),
        scratch_shapes=[pltpu.VMEM((experts, block), f32), dma((experts,)), dma(()), dma(())],
        cost_estimate=pl.CostEstimate(flops=0, bytes_accessed=4 * experts * block * cols * shards, transcendentals=0),
        compiler_params=pltpu.CompilerParams(vmem_limit_bytes=4 * 2**20),
    )(landed, scale, serve)
    if late:
        ready = pl.pallas_call(
            functools.partial(add_last, shards),
            out_shape=jax.ShapeDtypeStruct(ready.shape, bf16),
            in_specs=[hbm, vmem],
            out_specs=hbm,
            input_output_aliases={0: 0},
            scratch_shapes=[dma(())],
            compiler_params=pltpu.CompilerParams(vmem_limit_bytes=4 * 2**20),
        )(ready, last)
    return ready, scale, serve.T


def solution(mesh):
    in_specs = (
        P("expert", None, "shard"),
        P("expert", None, "shard"),
        P("shard", "expert"),
        P("shard"),
    )
    out_specs = (P("expert", "shard", None), P("expert", "shard"), P())
    body = functools.partial(per_device, mesh.shape["expert"], mesh.shape["shard"])
    return jax.shard_map(
        body, mesh=mesh, in_specs=in_specs, out_specs=out_specs, check_vma=False
    )
```

```python
import functools

import jax
import jax.numpy as jnp
from jax import lax
from jax.experimental import pallas as pl
from jax.experimental.pallas import tpu as pltpu
from jax.sharding import PartitionSpec as P

MESH = pl.DeviceIdType.MESH
AHEAD = 3
DEPTH = 10
DIRECT = 1
SOON = 1
EARLY = 2
LATE = 192
LANES = 128


def exchange(
    groups, shards, parts, direct, late,
    train, other, router, gain,
    ready, scale_out, serve, last,
    tbuf, obuf, stage, lmax, amax, rmax, hown, xmax, gown, gmax, rparts, rflip,
    tsem, osem, data_send, data_recv, a_send, a_recv,
    p1_send, p1_recv, p2_send, p2_recv, p3_send, p3_recv,
    r1_send, r1_recv, r2_send, r2_recv, r3_send, r3_recv,
):
    me = lax.axis_index("shard")
    group = lax.axis_index("expert")
    experts = train.shape[0]
    slots, _, rows, cols = tbuf.shape
    depth = stage.shape[0]
    total = experts * parts * rows
    chunks = experts * parts
    block = rows * parts
    half = shards // 2
    side, seat = me // half, lax.rem(me, half)

    def shard_id(k):
        return lax.rem(me + k, shards)

    def group_id(k):
        return lax.rem(group + k, groups)

    def seat_id(k):
        return lax.rem(seat + k, half)

    across = lax.rem(me + half, shards)
    kept = {}
    for c in range(chunks - 1, -1, -1):
        left = max(0, min(rows, total - late - c * rows))
        if left < rows:
            kept[c] = left

    def held(c, b):
        if c in kept:
            return stage.at[b, pl.ds(0, (shards - 2) * rows + kept[c])]
        return stage.at[b, pl.ds(0, (shards - 1) * rows)]

    barrier = pltpu.get_barrier_semaphore()
    for k in range(1, shards):
        pl.semaphore_signal(barrier, inc=1, device_id=(group, shard_id(k)), device_id_type=MESH)
    for k in range(1, groups):
        pl.semaphore_signal(barrier, inc=1, device_id=(group_id(k), me), device_id_type=MESH)

    def place(c, d):
        return c // parts, pl.ds(pl.multiple_of(d * block + lax.rem(c, parts) * rows, 8), rows)

    def load(c, d):
        e, span = place(c, d)
        slot = lax.rem(c, slots)
        return (
            pltpu.make_async_copy(train.at[e, span], tbuf.at[slot, d], tsem.at[slot, d]),
            pltpu.make_async_copy(other.at[e, span], obuf.at[slot, d], osem.at[slot, d]),
        )

    def start_load(c):
        def one(d, _):
            for copy in load(c, d):
                copy.start()
            return 0
        lax.fori_loop(0, shards, one, 0)

    def columns_of(d):
        return pl.ds(pl.multiple_of(d * cols, LANES), cols)

    def send(src, dst, send_sem, recv_sem, peer):
        return pltpu.make_async_remote_copy(
            src_ref=src, dst_ref=dst, send_sem=send_sem, recv_sem=recv_sem,
            device_id=(group, peer), device_id_type=MESH,
        )

    def wait_for(some, sem):
        pltpu.make_async_copy(some, some, sem).wait()

    def find_max(c):
        slot = lax.rem(c, slots)

        def one(d, _):
            for copy in load(c, d):
                copy.wait()
            best = None
            for j in range(0, cols, LANES):
                at = pl.ds(j, LANES)
                now = jnp.abs(tbuf[slot, d, :, at] + obuf[slot, d, :, at].astype(jnp.float32))
                best = now if best is None else jnp.maximum(best, now)
            lmax[c, d // half, lax.rem(d, half)] = jnp.max(best.T, axis=0, keepdims=True)
            return 0
        lax.fori_loop(0, shards, one, 0)

    def tell_all(c):
        def tell(k, _):
            send(lmax.at[c], amax.at[c, me], a_send.at[c], a_recv.at[c], shard_id(k)).start()
            return 0
        lax.fori_loop(1, shards, tell, 0)
        amax[c, me] = lmax[c]

    def hear_all(c):
        wait_for(amax.at[c, pl.ds(0, shards - 1)], a_recv.at[c])
        best = amax[c, 0]
        for d in range(1, shards):
            best = jnp.maximum(best, amax[c, d])
        for j in range(half):
            gmax[c, j] = best[:, j]

    def tell_leaders(c):
        def tell(k, _):
            j = seat_id(k)
            send(lmax.at[c, :, j], rmax.at[c, seat], p1_send.at[c], p1_recv.at[c], side * half + j).start()
            return 0
        lax.fori_loop(1, half, tell, 0)
        rmax[c, seat] = lmax[c, :, seat]

    def tell_across(c):
        wait_for(rmax.at[c, pl.ds(0, half - 1)], p1_recv.at[c])
        best = rmax[c, 0]
        for j in range(1, half):
            best = jnp.maximum(best, rmax[c, j])
        hown[c] = best
        send(hown.at[c], xmax.at[c], p2_send.at[c], p2_recv.at[c], across).start()

    def tell_half(c):
        wait_for(xmax.at[c], p2_recv.at[c])
        best = jnp.maximum(hown[c], xmax[c])
        gown[c] = best

        def tell(k, _):
            send(gown.at[c], gmax.at[c, seat], p3_send.at[c], p3_recv.at[c], side * half + seat_id(k)).start()
            return 0
        lax.fori_loop(1, half, tell, 0)
        gmax[c, seat] = best

    def open_chunk(c):
        berth = lax.rem(c, depth)

        @pl.when(c < direct)
        def _():
            hear_all(c)

        @pl.when(c >= direct)
        def _():
            wait_for(gmax.at[c, pl.ds(0, half - 1)], p3_recv.at[c])

        @pl.when(c >= depth)
        def _():
            wait_for(held(None, berth), data_send.at[berth])
        scale_out[c] = gmax[c, seat, side]

    def narrow(c, begin, end):
        slot = lax.rem(c, slots)
        berth = lax.rem(c, depth)
        first = pl.multiple_of(c * rows, 8)

        def one(k, _):
            d = lax.rem(me + half + half * lax.rem(c, 2) + k, shards)
            tall = jnp.broadcast_to(gmax[c, lax.rem(d, half), d // half], (LANES, rows)).T
            for j in range(0, cols, LANES):
                at = pl.ds(j, LANES)
                now = tbuf[slot, d, :, at] + obuf[slot, d, :, at].astype(jnp.float32)
                stage[berth, pl.ds(pl.multiple_of(d * rows, 8), rows), at] = (now / tall).astype(jnp.bfloat16)

            def part(count):
                send(
                    stage.at[berth, pl.ds(pl.multiple_of(d * rows, 8), count)],
                    ready.at[pl.ds(first, count), columns_of(me)],
                    data_send.at[berth], data_recv.at[me], d,
                ).start()

            whole = d != me
            for special in kept:
                whole = whole & ((d != across) | (c != special))

            @pl.when(whole)
            def _():
                part(rows)

            for special, left in kept.items():
                @pl.when((d == across) & (c == special))
                def _():
                    if left:
                        part(left)
                    at = special * rows + left - (total - late)
                    last[at:at + rows - left, :] = stage[berth, pl.ds(pl.multiple_of(d * rows + left, 8), rows - left), :]

            @pl.when(d == me)
            def _():
                ready[pl.ds(first, rows), columns_of(me)] = stage[berth, pl.ds(pl.multiple_of(d * rows, 8), rows), :]
            return 0
        lax.fori_loop(begin, end, one, 0)

    for c in range(min(AHEAD, chunks)):
        start_load(c)
    for c in range(min(SOON, chunks)):
        find_max(c)
    for c in range(AHEAD, min(AHEAD + 2, chunks)):
        start_load(c)
    rparts[group, side, seat] = router[...] * gain[...]
    pl.semaphore_wait(barrier, shards - 1 + groups - 1)
    for c in range(min(AHEAD, chunks)):
        if c >= SOON:
            find_max(c)
        if c < direct:
            tell_all(c)
        else:
            tell_leaders(c)
    mine = rparts.at[group, side, seat]
    send(mine, mine, r1_send, r1_recv, across).start()
    for c in range(direct, min(AHEAD - 1, chunks)):
        tell_across(c)
    open_chunk(0)
    narrow(0, 0, EARLY)

    def step(c, _):
        @pl.when(c < chunks)
        def _():
            find_max(c)
            tell_leaders(c)

        @pl.when((c >= max(direct + 1, AHEAD)) & (c <= chunks))
        def _():
            tell_across(c - 1)

        @pl.when((c >= direct + 2) & (c <= chunks + 1))
        def _():
            tell_half(c - 2)

        @pl.when(c == AHEAD)
        def _():
            wait_for(mine, r1_recv)
            for k in range(1, half):
                both = rparts.at[group, :, seat]
                send(both, both, r2_send, r2_recv, side * half + seat_id(k)).start()

        @pl.when(c == min(AHEAD + 1, chunks + AHEAD - 1))
        def _():
            wait_for(rparts.at[group, :, pl.ds(0, half - 1)], r2_recv)
            for k in range(1, groups):
                pltpu.make_async_remote_copy(
                    src_ref=rparts.at[group], dst_ref=rparts.at[group], send_sem=r3_send, recv_sem=r3_recv,
                    device_id=(group_id(k), me), device_id_type=MESH,
                ).start()

        @pl.when(c > AHEAD)
        def _():
            open_chunk(c - AHEAD)
        narrow(c - AHEAD, jnp.where(c == AHEAD, EARLY, 0), shards)

        @pl.when(c + 2 < chunks)
        def _():
            start_load(c + 2)
        return 0

    lax.fori_loop(AHEAD, chunks + AHEAD, step, 0)

    wait_for(rparts.at[pl.ds(0, groups - 1)], r3_recv)
    wide = router.shape[1]
    for d in range(shards):
        for g in range(groups):
            rflip[g * experts:(g + 1) * experts, :] = rparts[g, d // half, d % half]
        serve[:, d * wide:(d + 1) * wide] = rflip[...].astype(jnp.bfloat16)

    wait_for(mine, r1_send)
    wait_for(rparts.at[group, :, pl.ds(0, half - 1)], r2_send)
    wait_for(rparts.at[pl.ds(0, groups - 1)], r3_send)
    for c in range(direct):
        wait_for(amax.at[c, pl.ds(0, shards - 1)], a_send.at[c])

    def drain(c, _):
        wait_for(rmax.at[c, pl.ds(0, half - 1)], p1_send.at[c])
        wait_for(xmax.at[c], p2_send.at[c])
        wait_for(gmax.at[c, pl.ds(0, half - 1)], p3_send.at[c])
        return 0
    lax.fori_loop(direct, chunks, drain, 0)

    for c in range(chunks - depth, chunks):
        wait_for(held(c, c % depth), data_send.at[c % depth])

    wait_for(ready.at[pl.ds(0, total - late), columns_of(across)], data_recv.at[across])

    def finish(k, _):
        d = lax.rem(across + k, shards)

        @pl.when(d != me)
        def _():
            wait_for(ready.at[:, columns_of(d)], data_recv.at[d])
        return 0
    lax.fori_loop(1, shards, finish, 0)


def write_out(parts, landed, scale_in, serve_in, ready, scale, serve, rows_of, sem, scale_sem, serve_sem):
    experts, block, _ = ready.shape
    rows = block // parts
    for e in range(experts):
        for p in range(parts):
            span = pl.ds(p * rows, rows)
            pltpu.make_async_copy(landed.at[pl.ds(e * block + p * rows, rows)], ready.at[e, span], sem.at[e]).start()
    pltpu.make_async_copy(serve_in, serve, serve_sem).start()
    for e in range(experts):
        rows_of[e:e + 1, :] = jnp.concatenate([scale_in[e * parts + p] for p in range(parts)], axis=1)
    pltpu.make_async_copy(rows_of, scale, scale_sem).start()
    pltpu.make_async_copy(serve_in, serve, serve_sem).wait()
    pltpu.make_async_copy(rows_of, scale, scale_sem).wait()
    for e in range(experts):
        pltpu.make_async_copy(landed.at[pl.ds(e * block, block)], ready.at[e], sem.at[e]).wait()


def add_last(shards, ready_in, last, ready, sem):
    late, cols = last.shape
    experts, block, _ = ready.shape
    across = lax.rem(lax.axis_index("shard") + shards // 2, shards)
    copy = pltpu.make_async_copy(
        last, ready.at[experts - 1, pl.ds(block - late, late), pl.ds(pl.multiple_of(across * cols, LANES), cols)], sem
    )
    copy.start()
    copy.wait()


def pieces(block):
    for count in (5, 4, 3, 2):
        if block % (16 * count) == 0:
            return count
    return 1


def per_device(groups, shards, train_down, other_down, router_weight, router_gain):
    experts, height, cols = train_down.shape
    block = height // shards
    parts = pieces(block)
    rows = block // parts
    chunks = experts * parts
    direct = min(DIRECT, chunks)
    slots = AHEAD + 2
    depth = min(DEPTH, chunks)
    half = shards // 2
    wide = router_weight.shape[0]
    late = LATE if chunks > depth and LATE < block else 0
    f32, bf16 = jnp.float32, jnp.bfloat16
    dma = pltpu.SemaphoreType.DMA
    hbm = pl.BlockSpec(memory_space=pl.ANY)
    vmem = pl.BlockSpec(memory_space=pltpu.VMEM)
    landed, scale, serve, last = pl.pallas_call(
        functools.partial(exchange, groups, shards, parts, direct, late),
        out_shape=(
            pltpu.VMEM((experts * block, cols * shards), bf16),
            pltpu.VMEM((chunks, 1, rows), f32),
            pltpu.VMEM((experts * groups, wide * shards), bf16),
            pltpu.VMEM((max(late, 16), cols), bf16),
        ),
        in_specs=[hbm, hbm, vmem, vmem],
        out_specs=(vmem, vmem, vmem, vmem),
        scratch_shapes=[
            pltpu.VMEM((slots, shards, rows, cols), f32),
            pltpu.VMEM((slots, shards, rows, cols), bf16),
            pltpu.VMEM((depth, shards * rows, cols), bf16),
            pltpu.VMEM((chunks, 2, half, 1, rows), f32),
            pltpu.VMEM((direct, shards, 2, half, 1, rows), f32),
            pltpu.VMEM((chunks, half, 2, 1, rows), f32),
            pltpu.VMEM((chunks, 2, 1, rows), f32),
            pltpu.VMEM((chunks, 2, 1, rows), f32),
            pltpu.VMEM((chunks, 2, 1, rows), f32),
            pltpu.VMEM((chunks, half, 2, 1, rows), f32),
            pltpu.VMEM((groups, 2, half, experts, wide), f32),
            pltpu.VMEM((groups * experts, wide), f32),
            dma((slots, shards)), dma((slots, shards)),
            dma((depth,)), dma((shards,)),
            dma((direct,)), dma((direct,)),
            dma((chunks,)), dma((chunks,)), dma((chunks,)), dma((chunks,)), dma((chunks,)), dma((chunks,)),
            dma(()), dma(()), dma(()), dma(()), dma(()), dma(()),
        ],
        compiler_params=pltpu.CompilerParams(
            collective_id=0, has_side_effects=True, vmem_limit_bytes=36 * 2**20
        ),
    )(train_down, other_down, router_weight.T, router_gain[None, :])
    if late:
        swap = [(d, (d + half) % shards) for d in range(shards)]
        last = lax.ppermute(last, "shard", swap)
    ready, scale, serve = pl.pallas_call(
        functools.partial(write_out, parts),
        out_shape=(
            jax.ShapeDtypeStruct((experts, block, cols * shards), bf16),
            jax.ShapeDtypeStruct((experts, block), f32),
            jax.ShapeDtypeStruct((experts * groups, wide * shards), bf16),
        ),
        in_specs=[vmem, vmem, vmem],
        out_specs=(hbm, hbm, hbm),
        scratch_shapes=[pltpu.VMEM((experts, block), f32), dma((experts,)), dma(()), dma(())],
        cost_estimate=pl.CostEstimate(flops=0, bytes_accessed=4 * experts * block * cols * shards, transcendentals=0),
        compiler_params=pltpu.CompilerParams(vmem_limit_bytes=4 * 2**20),
    )(landed, scale, serve)
    if late:
        ready = pl.pallas_call(
            functools.partial(add_last, shards),
            out_shape=jax.ShapeDtypeStruct(ready.shape, bf16),
            in_specs=[hbm, vmem],
            out_specs=hbm,
            input_output_aliases={0: 0},
            scratch_shapes=[dma(())],
            compiler_params=pltpu.CompilerParams(vmem_limit_bytes=4 * 2**20),
        )(ready, last)
    return ready, scale, serve.T


def solution(mesh):
    in_specs = (
        P("expert", None, "shard"),
        P("expert", None, "shard"),
        P("shard", "expert"),
        P("shard"),
    )
    out_specs = (P("expert", "shard", None), P("expert", "shard"), P())
    body = functools.partial(per_device, mesh.shape["expert"], mesh.shape["shard"])
    return jax.shard_map(
        body, mesh=mesh, in_specs=in_specs, out_specs=out_specs, check_vma=False
    )
```

```python
import functools

import jax
import jax.numpy as jnp
from jax import lax
from jax.experimental import pallas as pl
from jax.experimental.pallas import tpu as pltpu
from jax.sharding import PartitionSpec as P

MESH = pl.DeviceIdType.MESH
AHEAD = 3
DEPTH = 10
DIRECT = 1
SOON = 1
EARLY = 1
LATE = 192
LANES = 128


def exchange(
    groups, shards, parts, direct, late,
    train, other, router, gain,
    ready, scale_out, serve, last,
    tbuf, obuf, stage, lmax, amax, rmax, hown, xmax, gown, gmax, rparts, rflip,
    tsem, osem, data_send, data_recv, a_send, a_recv,
    p1_send, p1_recv, p2_send, p2_recv, p3_send, p3_recv,
    r1_send, r1_recv, r2_send, r2_recv, r3_send, r3_recv,
):
    me = lax.axis_index("shard")
    group = lax.axis_index("expert")
    experts = train.shape[0]
    slots, _, rows, cols = tbuf.shape
    depth = stage.shape[0]
    total = experts * parts * rows
    chunks = experts * parts
    block = rows * parts
    half = shards // 2
    side, seat = me // half, lax.rem(me, half)

    def shard_id(k):
        return lax.rem(me + k, shards)

    def group_id(k):
        return lax.rem(group + k, groups)

    def seat_id(k):
        return lax.rem(seat + k, half)

    across = lax.rem(me + half, shards)
    kept = {}
    for c in range(chunks - 1, -1, -1):
        left = max(0, min(rows, total - late - c * rows))
        if left < rows:
            kept[c] = left

    def held(c, b):
        if c in kept:
            return stage.at[b, pl.ds(0, (shards - 2) * rows + kept[c])]
        return stage.at[b, pl.ds(0, (shards - 1) * rows)]

    barrier = pltpu.get_barrier_semaphore()
    for k in range(1, shards):
        pl.semaphore_signal(barrier, inc=1, device_id=(group, shard_id(k)), device_id_type=MESH)
    for k in range(1, groups):
        pl.semaphore_signal(barrier, inc=1, device_id=(group_id(k), me), device_id_type=MESH)

    def place(c, d):
        return c // parts, pl.ds(pl.multiple_of(d * block + lax.rem(c, parts) * rows, 8), rows)

    def load(c, d):
        e, span = place(c, d)
        slot = lax.rem(c, slots)
        return (
            pltpu.make_async_copy(train.at[e, span], tbuf.at[slot, d], tsem.at[slot, d]),
            pltpu.make_async_copy(other.at[e, span], obuf.at[slot, d], osem.at[slot, d]),
        )

    def start_load(c):
        def one(d, _):
            for copy in load(c, d):
                copy.start()
            return 0
        lax.fori_loop(0, shards, one, 0)

    def columns_of(d):
        return pl.ds(pl.multiple_of(d * cols, LANES), cols)

    def send(src, dst, send_sem, recv_sem, peer):
        return pltpu.make_async_remote_copy(
            src_ref=src, dst_ref=dst, send_sem=send_sem, recv_sem=recv_sem,
            device_id=(group, peer), device_id_type=MESH,
        )

    def wait_for(some, sem):
        pltpu.make_async_copy(some, some, sem).wait()

    def find_max(c):
        slot = lax.rem(c, slots)

        def one(d, _):
            for copy in load(c, d):
                copy.wait()
            best = None
            for j in range(0, cols, LANES):
                at = pl.ds(j, LANES)
                now = jnp.abs(tbuf[slot, d, :, at] + obuf[slot, d, :, at].astype(jnp.float32))
                best = now if best is None else jnp.maximum(best, now)
            lmax[c, d // half, lax.rem(d, half)] = jnp.max(best.T, axis=0, keepdims=True)
            return 0
        lax.fori_loop(0, shards, one, 0)

    def tell_all(c):
        def tell(k, _):
            send(lmax.at[c], amax.at[c, me], a_send.at[c], a_recv.at[c], shard_id(k)).start()
            return 0
        lax.fori_loop(1, shards, tell, 0)
        amax[c, me] = lmax[c]

    def hear_all(c):
        wait_for(amax.at[c, pl.ds(0, shards - 1)], a_recv.at[c])
        best = amax[c, 0]
        for d in range(1, shards):
            best = jnp.maximum(best, amax[c, d])
        for j in range(half):
            gmax[c, j] = best[:, j]

    def tell_leaders(c):
        def tell(k, _):
            j = seat_id(k)
            send(lmax.at[c, :, j], rmax.at[c, seat], p1_send.at[c], p1_recv.at[c], side * half + j).start()
            return 0
        lax.fori_loop(1, half, tell, 0)
        rmax[c, seat] = lmax[c, :, seat]

    def tell_across(c):
        wait_for(rmax.at[c, pl.ds(0, half - 1)], p1_recv.at[c])
        best = rmax[c, 0]
        for j in range(1, half):
            best = jnp.maximum(best, rmax[c, j])
        hown[c] = best
        send(hown.at[c], xmax.at[c], p2_send.at[c], p2_recv.at[c], across).start()

    def tell_half(c):
        wait_for(xmax.at[c], p2_recv.at[c])
        best = jnp.maximum(hown[c], xmax[c])
        gown[c] = best

        def tell(k, _):
            send(gown.at[c], gmax.at[c, seat], p3_send.at[c], p3_recv.at[c], side * half + seat_id(k)).start()
            return 0
        lax.fori_loop(1, half, tell, 0)
        gmax[c, seat] = best

    def open_chunk(c):
        berth = lax.rem(c, depth)

        @pl.when(c < direct)
        def _():
            hear_all(c)

        @pl.when(c >= direct)
        def _():
            wait_for(gmax.at[c, pl.ds(0, half - 1)], p3_recv.at[c])

        @pl.when(c >= depth)
        def _():
            wait_for(held(None, berth), data_send.at[berth])
        scale_out[c] = gmax[c, seat, side]

    def narrow(c, begin, end):
        slot = lax.rem(c, slots)
        berth = lax.rem(c, depth)
        first = pl.multiple_of(c * rows, 8)

        def one(k, _):
            d = lax.rem(me + half + half * lax.rem(c, 2) + k, shards)
            tall = jnp.broadcast_to(gmax[c, lax.rem(d, half), d // half], (LANES, rows)).T
            for j in range(0, cols, LANES):
                at = pl.ds(j, LANES)
                now = tbuf[slot, d, :, at] + obuf[slot, d, :, at].astype(jnp.float32)
                stage[berth, pl.ds(pl.multiple_of(d * rows, 8), rows), at] = (now / tall).astype(jnp.bfloat16)

            def part(count):
                send(
                    stage.at[berth, pl.ds(pl.multiple_of(d * rows, 8), count)],
                    ready.at[pl.ds(first, count), columns_of(me)],
                    data_send.at[berth], data_recv.at[me], d,
                ).start()

            whole = d != me
            for special in kept:
                whole = whole & ((d != across) | (c != special))

            @pl.when(whole)
            def _():
                part(rows)

            for special, left in kept.items():
                @pl.when((d == across) & (c == special))
                def _():
                    if left:
                        part(left)
                    at = special * rows + left - (total - late)
                    last[at:at + rows - left, :] = stage[berth, pl.ds(pl.multiple_of(d * rows + left, 8), rows - left), :]

            @pl.when(d == me)
            def _():
                ready[pl.ds(first, rows), columns_of(me)] = stage[berth, pl.ds(pl.multiple_of(d * rows, 8), rows), :]
            return 0
        lax.fori_loop(begin, end, one, 0)

    for c in range(min(AHEAD, chunks)):
        start_load(c)
    for c in range(min(SOON, chunks)):
        find_max(c)
    for c in range(AHEAD, min(AHEAD + 2, chunks)):
        start_load(c)
    rparts[group, side, seat] = router[...] * gain[...]
    pl.semaphore_wait(barrier, shards - 1 + groups - 1)
    for c in range(min(AHEAD, chunks)):
        if c >= SOON:
            find_max(c)
        if c < direct:
            tell_all(c)
        else:
            tell_leaders(c)
    mine = rparts.at[group, side, seat]
    send(mine, mine, r1_send, r1_recv, across).start()
    for c in range(direct, min(AHEAD - 1, chunks)):
        tell_across(c)
    open_chunk(0)
    narrow(0, 0, EARLY)

    def step(c, _):
        @pl.when(c < chunks)
        def _():
            find_max(c)
            tell_leaders(c)

        @pl.when((c >= max(direct + 1, AHEAD)) & (c <= chunks))
        def _():
            tell_across(c - 1)

        @pl.when((c >= direct + 2) & (c <= chunks + 1))
        def _():
            tell_half(c - 2)

        @pl.when(c == AHEAD)
        def _():
            wait_for(mine, r1_recv)
            for k in range(1, half):
                both = rparts.at[group, :, seat]
                send(both, both, r2_send, r2_recv, side * half + seat_id(k)).start()

        @pl.when(c == min(AHEAD + 1, chunks + AHEAD - 1))
        def _():
            wait_for(rparts.at[group, :, pl.ds(0, half - 1)], r2_recv)
            for k in range(1, groups):
                pltpu.make_async_remote_copy(
                    src_ref=rparts.at[group], dst_ref=rparts.at[group], send_sem=r3_send, recv_sem=r3_recv,
                    device_id=(group_id(k), me), device_id_type=MESH,
                ).start()

        @pl.when(c > AHEAD)
        def _():
            open_chunk(c - AHEAD)
        narrow(c - AHEAD, jnp.where(c == AHEAD, EARLY, 0), shards)

        @pl.when(c + 2 < chunks)
        def _():
            start_load(c + 2)
        return 0

    lax.fori_loop(AHEAD, chunks + AHEAD, step, 0)

    wait_for(rparts.at[pl.ds(0, groups - 1)], r3_recv)
    wide = router.shape[1]
    for d in range(shards):
        for g in range(groups):
            rflip[g * experts:(g + 1) * experts, :] = rparts[g, d // half, d % half]
        serve[:, d * wide:(d + 1) * wide] = rflip[...].astype(jnp.bfloat16)

    wait_for(mine, r1_send)
    wait_for(rparts.at[group, :, pl.ds(0, half - 1)], r2_send)
    wait_for(rparts.at[pl.ds(0, groups - 1)], r3_send)
    for c in range(direct):
        wait_for(amax.at[c, pl.ds(0, shards - 1)], a_send.at[c])

    def drain(c, _):
        wait_for(rmax.at[c, pl.ds(0, half - 1)], p1_send.at[c])
        wait_for(xmax.at[c], p2_send.at[c])
        wait_for(gmax.at[c, pl.ds(0, half - 1)], p3_send.at[c])
        return 0
    lax.fori_loop(direct, chunks, drain, 0)

    for c in range(chunks - depth, chunks):
        wait_for(held(c, c % depth), data_send.at[c % depth])

    wait_for(ready.at[pl.ds(0, total - late), columns_of(across)], data_recv.at[across])

    def finish(k, _):
        d = lax.rem(across + k, shards)

        @pl.when(d != me)
        def _():
            wait_for(ready.at[:, columns_of(d)], data_recv.at[d])
        return 0
    lax.fori_loop(1, shards, finish, 0)


def write_out(parts, landed, scale_in, serve_in, ready, scale, serve, rows_of, sem, scale_sem, serve_sem):
    experts, block, _ = ready.shape
    rows = block // parts
    for e in range(experts):
        for p in range(parts):
            span = pl.ds(p * rows, rows)
            pltpu.make_async_copy(landed.at[pl.ds(e * block + p * rows, rows)], ready.at[e, span], sem.at[e]).start()
    pltpu.make_async_copy(serve_in, serve, serve_sem).start()
    for e in range(experts):
        rows_of[e:e + 1, :] = jnp.concatenate([scale_in[e * parts + p] for p in range(parts)], axis=1)
    pltpu.make_async_copy(rows_of, scale, scale_sem).start()
    pltpu.make_async_copy(serve_in, serve, serve_sem).wait()
    pltpu.make_async_copy(rows_of, scale, scale_sem).wait()
    for e in range(experts):
        pltpu.make_async_copy(landed.at[pl.ds(e * block, block)], ready.at[e], sem.at[e]).wait()


def add_last(shards, ready_in, last, ready, sem):
    late, cols = last.shape
    experts, block, _ = ready.shape
    across = lax.rem(lax.axis_index("shard") + shards // 2, shards)
    copy = pltpu.make_async_copy(
        last, ready.at[experts - 1, pl.ds(block - late, late), pl.ds(pl.multiple_of(across * cols, LANES), cols)], sem
    )
    copy.start()
    copy.wait()


def pieces(block):
    for count in (5, 4, 3, 2):
        if block % (16 * count) == 0:
            return count
    return 1


def per_device(groups, shards, train_down, other_down, router_weight, router_gain):
    experts, height, cols = train_down.shape
    block = height // shards
    parts = pieces(block)
    rows = block // parts
    chunks = experts * parts
    direct = min(DIRECT, chunks)
    slots = AHEAD + 2
    depth = min(DEPTH, chunks)
    half = shards // 2
    wide = router_weight.shape[0]
    late = LATE if chunks > depth and LATE < block else 0
    f32, bf16 = jnp.float32, jnp.bfloat16
    dma = pltpu.SemaphoreType.DMA
    hbm = pl.BlockSpec(memory_space=pl.ANY)
    vmem = pl.BlockSpec(memory_space=pltpu.VMEM)
    landed, scale, serve, last = pl.pallas_call(
        functools.partial(exchange, groups, shards, parts, direct, late),
        out_shape=(
            pltpu.VMEM((experts * block, cols * shards), bf16),
            pltpu.VMEM((chunks, 1, rows), f32),
            pltpu.VMEM((experts * groups, wide * shards), bf16),
            pltpu.VMEM((max(late, 16), cols), bf16),
        ),
        in_specs=[hbm, hbm, vmem, vmem],
        out_specs=(vmem, vmem, vmem, vmem),
        scratch_shapes=[
            pltpu.VMEM((slots, shards, rows, cols), f32),
            pltpu.VMEM((slots, shards, rows, cols), bf16),
            pltpu.VMEM((depth, shards * rows, cols), bf16),
            pltpu.VMEM((chunks, 2, half, 1, rows), f32),
            pltpu.VMEM((direct, shards, 2, half, 1, rows), f32),
            pltpu.VMEM((chunks, half, 2, 1, rows), f32),
            pltpu.VMEM((chunks, 2, 1, rows), f32),
            pltpu.VMEM((chunks, 2, 1, rows), f32),
            pltpu.VMEM((chunks, 2, 1, rows), f32),
            pltpu.VMEM((chunks, half, 2, 1, rows), f32),
            pltpu.VMEM((groups, 2, half, experts, wide), f32),
            pltpu.VMEM((groups * experts, wide), f32),
            dma((slots, shards)), dma((slots, shards)),
            dma((depth,)), dma((shards,)),
            dma((direct,)), dma((direct,)),
            dma((chunks,)), dma((chunks,)), dma((chunks,)), dma((chunks,)), dma((chunks,)), dma((chunks,)),
            dma(()), dma(()), dma(()), dma(()), dma(()), dma(()),
        ],
        compiler_params=pltpu.CompilerParams(
            collective_id=0, has_side_effects=True, vmem_limit_bytes=36 * 2**20
        ),
    )(train_down, other_down, router_weight.T, router_gain[None, :])
    if late:
        swap = [(d, (d + half) % shards) for d in range(shards)]
        last = lax.ppermute(last, "shard", swap)
    ready, scale, serve = pl.pallas_call(
        functools.partial(write_out, parts),
        out_shape=(
            jax.ShapeDtypeStruct((experts, block, cols * shards), bf16),
            jax.ShapeDtypeStruct((experts, block), f32),
            jax.ShapeDtypeStruct((experts * groups, wide * shards), bf16),
        ),
        in_specs=[vmem, vmem, vmem],
        out_specs=(hbm, hbm, hbm),
        scratch_shapes=[pltpu.VMEM((experts, block), f32), dma((experts,)), dma(()), dma(())],
        cost_estimate=pl.CostEstimate(flops=0, bytes_accessed=4 * experts * block * cols * shards, transcendentals=0),
        compiler_params=pltpu.CompilerParams(vmem_limit_bytes=4 * 2**20),
    )(landed, scale, serve)
    if late:
        ready = pl.pallas_call(
            functools.partial(add_last, shards),
            out_shape=jax.ShapeDtypeStruct(ready.shape, bf16),
            in_specs=[hbm, vmem],
            out_specs=hbm,
            input_output_aliases={0: 0},
            scratch_shapes=[dma(())],
            compiler_params=pltpu.CompilerParams(vmem_limit_bytes=4 * 2**20),
        )(ready, last)
    return ready, scale, serve.T


def solution(mesh):
    in_specs = (
        P("expert", None, "shard"),
        P("expert", None, "shard"),
        P("shard", "expert"),
        P("shard"),
    )
    out_specs = (P("expert", "shard", None), P("expert", "shard"), P())
    body = functools.partial(per_device, mesh.shape["expert"], mesh.shape["shard"])
    return jax.shard_map(
        body, mesh=mesh, in_specs=in_specs, out_specs=out_specs, check_vma=False
    )
```
